32 devices in a mesh: member: 2 (over x), node: 16 (over z, y, core).
Axes of the slice: x: 2, y: 2, z: 4, core: 2. Of those that a mesh axis runs over, the one named last changes fastest.
Arguments:
- conditioning: bfloat16 [168, 32768], P(None, ('member', 'node')), parts along dimension 1, may hold values from -6 to 6
- target_state: float32 [84, 32768], P(None, ('member', 'node')), parts along dimension 1, may hold values from -6 to 6
- noise_sample: float32 [84, 32768], P(None, ('member', 'node')), parts along dimension 1, may hold values from -6 to 6
- step_index: int32 [2], P('member'), parts along dimension 0, may hold values from 0 to 19
- mesh_features: float32 [3, 10240], P(None, 'node'), may hold values from -1 to 1
- edge_geometry: float32 [4, 65536], P(None, 'node'), may hold values from -6 to 6
- edge_slot: int32 [65536], P('node'), may hold values from 0 to 255, as said below
- edge_receiver: int32 [65536], P('node'), may hold values from 0 to 639
- send_rows: int32 [256, 16], P('node'), may hold values from 0 to 1023
- edge_count: int32 [16], P('node'), may hold values from 1399 to 4096, as said below
- embed_weight: bfloat16 [252, 512], replicated, may hold values from -0.375 to 0.375
- mesh_weight: float32 [3, 512], replicated, may hold values from -3.5 to 3.5
- geom_weight: float32 [4, 512], replicated, may hold values from -3 to 3
- sender_weight: bfloat16 [512, 512], P('node'), may hold values from -0.15625 to 0.15625
- edge_weight: bfloat16 [512, 512], P('node'), may hold values from -0.15625 to 0.15625
- receiver_weight: bfloat16 [512, 512], P('node'), may hold values from -0.15625 to 0.15625
- message_weight: bfloat16 [512, 512], P('node'), may hold values from -0.25 to 0.25
- node_weight: bfloat16 [1024, 512], P('node'), may hold values from -0.1875 to 0.1875
- output_weight: bfloat16 [512, 512], P('node'), may hold values from -0.25 to 0.25
- noise_weight: float32 [32, 512], replicated, may hold values from -1 to 1
- film_weight: bfloat16 [512, 2048], replicated, may hold values from -0.25 to 0.25
Outputs:
- mesh_latent: bfloat16 [10240, 1024], P('node', 'member'), parts along dimension 1
The draws below stay inside these ranges and needn't reach their ends.
There are 2 independent parts, one for each index of `member`. The reference program is written for one: setup_inputs(seed, part) draws one part's arguments, and reference() takes and returns one part's arrays. A program takes and returns all parts, laid end to end along the dimension named above; an argument that names none is the same for every part. Nothing has to cross between parts.
Inputs may be any that keep to these rules, and one draw needn't show every extreme that they name: `edge_slot`: on each device, the live slots name every entry of its 16 * 16 list at least once, or as many distinct entries as there are live slots where these are fewer. `edge_count`: the counts sum to 16 * 2048 and one device has all 4096 slots live.
All inputs are finite; a program needn't handle non-finite values.
Results may differ from the reference program's by a relative error of at most 0.0071.
Values may be sent and summed in bfloat16 or wider, within the bound.
A program may use at most 64 MiB of HBM per device.

```python
import jax
import jax.numpy as jnp
from jax import lax

LAT = 512
VARS = 84
G_DEV = 1024
M_DEV = 640
E_DEV = 4096
CAP = 16
STEPS = 20
FREQ = 16
C_COND = 168
C_RAW = 252
GRID = 16384
MESH = 10240
EDGES = 65536
PAIRS = 256
N_NODE = 16


def live_counts(key):
    base_key = jax.random.fold_in(key, 11)
    order_key, spread_key = jax.random.split(base_key)
    order = jax.random.permutation(order_key, N_NODE).astype(jnp.int32)
    position = jnp.arange(N_NODE, dtype=jnp.int32)
    others = N_NODE - 1
    excess = E_DEV // 2
    share = excess // others
    remain = excess % others
    loss = share + (position - 1 < remain).astype(jnp.int32)
    spread = jax.random.randint(spread_key, (N_NODE,), 0, E_DEV // 8 + 1).astype(jnp.int32)
    following = jnp.where(position == N_NODE - 1, 1, position + 1).astype(jnp.int32)
    delta = spread - spread[following]
    placed = jnp.where(position == 0, E_DEV, E_DEV // 2 - loss + delta).astype(jnp.int32)
    return jnp.zeros((N_NODE,), jnp.int32).at[order].set(placed)


def draw_edge_count(key, part):
    return live_counts(key)


def draw_edge_slot(key, part):
    counts = live_counts(key)
    listed = N_NODE * CAP
    slot_key = jax.random.fold_in(key, 23)
    device_keys = jax.vmap(lambda index: jax.random.fold_in(slot_key, index))(jnp.arange(N_NODE, dtype=jnp.int32))

    def one_device(device_key, count):
        first_key, second_key = jax.random.split(device_key)
        order = jax.random.permutation(first_key, listed).astype(jnp.int32)
        extra = jax.random.randint(second_key, (E_DEV,), 0, listed).astype(jnp.int32)
        used = jnp.minimum(count, listed)
        position = jnp.arange(E_DEV, dtype=jnp.int32)
        pick = jnp.where(position < listed, position, extra % used)
        pick = jnp.minimum(pick, listed - 1)
        return order[pick]
    return jax.vmap(one_device)(device_keys, counts).reshape(N_NODE * E_DEV)


def plant(drawn, stream_key, smallest, high):
    longest = drawn.shape.index(max(drawn.shape))
    spots = []
    for shift in (0, 1):
        where = [jax.random.randint(jax.random.fold_in(stream_key, axis), (), 0, length) for axis, length in enumerate(drawn.shape)]
        where[longest] = (where[longest] + shift) % drawn.shape[longest]
        spots.append(tuple(where))
    return drawn.at[spots[0]].set(smallest).at[spots[1]].set(high)


def block_levels(key, shape, shards, least, largest):
    factor_of, own = 1.0, jax.random.fold_in(key, 6)
    for axis_at, blocks in shards:
        steps = jnp.exp(jax.random.uniform(jax.random.fold_in(own, axis_at), (blocks,), jnp.float32, least / len(shards), largest / len(shards)))
        factor_of = factor_of * jnp.repeat(steps, shape[axis_at] // blocks).reshape([-1 if axis == axis_at else 1 for axis in range(len(shape))])
    return factor_of


def gaussian(key, extent, width, limit, pieces=(), held_as=jnp.bfloat16):
    drawn = width * jax.random.normal(key, extent, jnp.float32)
    if pieces:
        drawn = drawn * block_levels(key, extent, pieces, -0.22, 0.18)
    return jnp.clip(drawn, -limit, limit).astype(held_as)


def setup_inputs(seed: int = 0, part: int = 0) -> dict:
    arg_keys = jax.random.split(jax.random.key(seed), 22)
    part_splits = jax.random.split(jax.random.fold_in(arg_keys[21], part), 22)
    return {
        "conditioning": gaussian(part_splits[0], (C_COND, GRID), 1.0, 6.0, ((1, 16),)),
        "target_state": gaussian(part_splits[1], (VARS, GRID), 1.0, 6.0, ((1, 16),), jnp.float32),
        "noise_sample": gaussian(part_splits[2], (VARS, GRID), 1.0, 6.0, ((1, 16),), jnp.float32),
        "step_index": jax.random.randint(part_splits[3], (1,), 0, STEPS).astype(jnp.int32),
        "mesh_features": jnp.clip(jax.random.uniform(arg_keys[4], (3, MESH), jnp.float32, -1.0, 1.0) * block_levels(arg_keys[4], (3, MESH), ((1, 16),), -0.4, 0.0), -1.0, 1.0),
        "edge_geometry": gaussian(arg_keys[5], (4, EDGES), 1.0, 6.0, ((1, 16),), jnp.float32),
        "edge_slot": draw_edge_slot(jax.random.fold_in(arg_keys[21], 71), part),
        "edge_receiver": plant(jax.random.randint(arg_keys[7], (EDGES,), 0, M_DEV), jax.random.fold_in(arg_keys[7], 1), 0, M_DEV - 1).astype(jnp.int32),
        "send_rows": plant(jax.random.randint(arg_keys[8], (PAIRS, CAP), 0, G_DEV), jax.random.fold_in(arg_keys[8], 1), 0, G_DEV - 1).astype(jnp.int32),
        "edge_count": draw_edge_count(jax.random.fold_in(arg_keys[21], 71), part),
        "embed_weight": gaussian(arg_keys[10], (C_RAW, LAT), C_RAW ** -0.5, 0.375),
        "mesh_weight": gaussian(arg_keys[11], (3, LAT), 3 ** -0.5, 3.5, (), jnp.float32),
        "geom_weight": gaussian(arg_keys[12], (4, LAT), 4 ** -0.5, 3.0, (), jnp.float32),
        "sender_weight": gaussian(arg_keys[13], (LAT, LAT), (3 * LAT) ** -0.5, 0.15625, ((0, 16),)),
        "edge_weight": gaussian(arg_keys[14], (LAT, LAT), (3 * LAT) ** -0.5, 0.15625, ((0, 16),)),
        "receiver_weight": gaussian(arg_keys[15], (LAT, LAT), (3 * LAT) ** -0.5, 0.15625, ((0, 16),)),
        "message_weight": gaussian(arg_keys[16], (LAT, LAT), LAT ** -0.5, 0.25, ((0, 16),)),
        "node_weight": gaussian(arg_keys[17], (2 * LAT, LAT), (2 * LAT) ** -0.5, 0.1875, ((0, 16),)),
        "output_weight": gaussian(arg_keys[18], (LAT, LAT), LAT ** -0.5, 0.25, ((0, 16),)),
        "noise_weight": gaussian(arg_keys[19], (2 * FREQ, LAT), (2 * FREQ) ** -0.5, 1.0, (), jnp.float32),
        "film_weight": gaussian(arg_keys[20], (LAT, 4 * LAT), LAT ** -0.5, 0.25),
    }


sigma_top = 80.0
sigma_low = 0.03
rho_power = 7.0
norm_eps = 1e-05

def layer_norm(values):
    mean = lax.optimization_barrier(jnp.mean(values, axis=-1, keepdims=True))
    centred = values - mean
    var = lax.optimization_barrier(jnp.mean(centred * centred, axis=-1, keepdims=True))
    return centred * lax.rsqrt(var + norm_eps)

def noise_terms(step_index, noise_weight, film_weight):
    frac = step_index[0].astype(jnp.float32) / (STEPS - 1)
    upper = sigma_top ** (1.0 / rho_power)
    lower = sigma_low ** (1.0 / rho_power)
    sigma = (upper + frac * (lower - upper)) ** rho_power
    angle = 0.25 * jnp.log(sigma) * (jnp.arange(FREQ, dtype=jnp.float32) + 1.0)
    fourier = jnp.concatenate([jnp.sin(angle), jnp.cos(angle)])[None, :]
    cond = jax.nn.silu(jnp.dot(fourier, noise_weight, precision=lax.Precision.HIGHEST)).astype(jnp.bfloat16)
    film = jnp.dot(cond, film_weight, preferred_element_type=jnp.float32)
    return (sigma, film)

def reference(conditioning, target_state, noise_sample, step_index, mesh_features, edge_geometry, edge_slot, edge_receiver, send_rows, edge_count, embed_weight, mesh_weight, geom_weight, sender_weight, edge_weight, receiver_weight, message_weight, node_weight, output_weight, noise_weight, film_weight):
    sigma, film = noise_terms(step_index, noise_weight, film_weight)
    edge_scale = film[:, 0:LAT]
    edge_shift = film[:, LAT:2 * LAT]
    node_scale = film[:, 2 * LAT:3 * LAT]
    node_shift = film[:, 3 * LAT:4 * LAT]
    noisy = ((target_state + sigma * noise_sample) / jnp.sqrt(sigma * sigma + 1.0)).astype(jnp.bfloat16)
    raw = jnp.concatenate([conditioning, noisy], axis=0)
    grid_latent = jax.nn.silu(jnp.dot(raw.T, embed_weight, preferred_element_type=jnp.float32)).astype(jnp.bfloat16)
    mesh_embed = jax.nn.silu(jnp.dot(mesh_features.T, mesh_weight, precision=lax.Precision.HIGHEST)).astype(jnp.bfloat16)
    recv_proj = jnp.dot(mesh_embed, receiver_weight, preferred_element_type=jnp.float32).astype(jnp.bfloat16)
    edge_embed = jax.nn.silu(jnp.dot(edge_geometry.T, geom_weight, precision=lax.Precision.HIGHEST)).astype(jnp.bfloat16)
    tables = send_rows.reshape(N_NODE, N_NODE, CAP)
    bands = jnp.arange(N_NODE, dtype=jnp.int32)

    def one_device(device):
        table = lax.dynamic_index_in_dim(tables, device, 1, keepdims=False)
        grid_index = (bands[:, None] * G_DEV + table).reshape(N_NODE * CAP)
        start = (device * E_DEV).astype(jnp.int32)
        slots = lax.dynamic_slice_in_dim(edge_slot, start, E_DEV, 0)
        local_recv = lax.dynamic_slice_in_dim(edge_receiver, start, E_DEV, 0)
        embed_rows = lax.dynamic_slice_in_dim(edge_embed, start, E_DEV, 0)
        node_start = (device * M_DEV).astype(jnp.int32)
        proj_local = lax.dynamic_slice_in_dim(recv_proj, node_start, M_DEV, 0)
        mesh_local = lax.dynamic_slice_in_dim(mesh_embed, node_start, M_DEV, 0)
        sender_rows = grid_latent[grid_index[slots]]
        pre = jnp.dot(embed_rows, edge_weight, preferred_element_type=jnp.float32)
        pre = pre + jnp.dot(sender_rows, sender_weight, preferred_element_type=jnp.float32)
        pre = pre + proj_local[local_recv].astype(jnp.float32)
        hidden = jax.nn.silu(pre).astype(jnp.bfloat16)
        mixed = jnp.dot(hidden, message_weight, preferred_element_type=jnp.float32)
        message = layer_norm(mixed) * (1.0 + edge_scale) + edge_shift
        count = lax.dynamic_index_in_dim(edge_count, device, 0, keepdims=False)
        live = jnp.arange(E_DEV, dtype=jnp.int32) < count
        message = jnp.where(live[:, None], message, 0.0).astype(jnp.bfloat16)
        gathered = jax.ops.segment_sum(message.astype(jnp.float32), local_recv, num_segments=M_DEV).astype(jnp.bfloat16)
        joined = jnp.concatenate([mesh_local, gathered], axis=1)
        update = jax.nn.silu(jnp.dot(joined, node_weight, preferred_element_type=jnp.float32)).astype(jnp.bfloat16)
        result = jnp.dot(update, output_weight, preferred_element_type=jnp.float32)
        return (mesh_local.astype(jnp.float32) + layer_norm(result) * (1.0 + node_scale) + node_shift).astype(jnp.bfloat16)
    blocks = lax.map(one_device, bands)
    return blocks.reshape(MESH, LAT)
```

```python
import functools

import jax
import jax.numpy as jnp
from jax import lax
from jax.experimental import pallas as pl
from jax.experimental.pallas import tpu as pltpu
from jax.sharding import PartitionSpec as P

STEPS = 20


sigma_top = 80.0
sigma_low = 0.03
rho_power = 7.0
norm_eps = 1e-05
f32, bf16 = jnp.float32, jnp.bfloat16


def is_folded(mesh):
    rows = mesh.devices[0]
    places = [getattr(device, "coords", None) for device in rows[:5:2]]
    if len(places) < 3 or any(place is None for place in places):
        return False
    first = [a != b for a, b in zip(places[0], places[1])]
    second = [a != b for a, b in zip(places[0], places[2])]
    return first != second


def silu(x):
    half = 0.5 * x
    return half * jnp.tanh(half) + half


def exchange_kernel(n, folded, *refs):
    shards, outgoing = refs[:6], refs[6]
    fulls, arrived = refs[7:13], refs[13]
    send_sem, recv_sem, psend_sem, precv_sem, asend_sem, arecv_sem, own_sem = refs[14:]
    me = lax.axis_index("node")
    core, chip = me % 2, me // 2
    partner = chip * 2 + 1 - core
    chips = n // 2
    half = chips // 2

    def swap(index):
        return index

    if folded:

        def to_pos(c):
            z, y = c // 2, c % 2
            return z + y * (chips - 1 - 2 * z)

        def to_chip(p):
            y = p // half
            return (p + y * (chips - 1 - 2 * p)) * 2 + y
    else:
        to_pos = to_chip = swap

    pos = to_pos(chip)

    def device_at(shift):
        return to_chip((pos + shift + chips) % chips) * 2 + core

    barrier = pltpu.get_barrier_semaphore()
    for step in range(1, n):
        pl.semaphore_signal(barrier, inc=1, device_id={"node": (me + step) % n})
    own = []
    for k in range(6):
        own.append(pltpu.make_async_copy(shards[k], fulls[k].at[me], own_sem.at[k]))
    own.append(pltpu.make_async_copy(outgoing.at[me], arrived.at[me], own_sem.at[6]))
    for copy in own:
        copy.start()
    pl.semaphore_wait(barrier, n - 1)

    sent = []
    waits = []

    def remote(source, target, send, recv, device):
        copy = pltpu.make_async_remote_copy(
            src_ref=source, dst_ref=target, send_sem=send, recv_sem=recv, device_id={"node": device}
        )
        copy.start()
        sent.append(copy)
        return copy

    for step in range(1, n):
        other = (me + step) % n
        waits.append(
            remote(outgoing.at[other], arrived.at[me], asend_sem.at[step], arecv_sem.at[step], other)
        )

    long, short = chips // 2, chips - 1 - chips // 2
    reach = [[long, short] if k % 2 == 0 else [short, long] for k in range(6)]
    ring = {}

    def pass_on(k, index, source, block):
        waits.append(
            remote(source, fulls[k].at[block], psend_sem.at[k, index], precv_sem.at[k, index], partner)
        )

    for step in range(1, long + 2):
        for k in range(6):
            for side in (0, 1):
                way = 1 - 2 * side
                last = reach[k][side]
                if step > last + 1:
                    continue
                block = device_at(-way * (step - 1))
                source = shards[k] if step == 1 else fulls[k].at[block]
                if step > 1:
                    ring[k, side, step - 1].wait_recv()
                if step <= last:
                    ring[k, side, step] = remote(
                        source,
                        fulls[k].at[block],
                        send_sem.at[k, side, step],
                        recv_sem.at[k, side, step],
                        device_at(way),
                    )
                if step > 1:
                    pass_on(k, side * (long + 1) + step - 1, source, block)
                elif side == 0:
                    pass_on(k, 0, source, block)
    for copy in waits:
        copy.wait_recv()
    for copy in sent:
        copy.wait_send()
    for copy in own:
        copy.wait()


def exchange(n, folded, shards, outgoing):
    long = n // 4 + 1
    outs = [jax.ShapeDtypeStruct((n,) + shard.shape, shard.dtype) for shard in shards]
    outs.append(jax.ShapeDtypeStruct(outgoing.shape, outgoing.dtype))
    dma = pltpu.SemaphoreType.DMA
    return pl.pallas_call(
        functools.partial(exchange_kernel, n, folded),
        out_shape=outs,
        in_specs=[pl.BlockSpec(memory_space=pltpu.VMEM)] * 7,
        out_specs=[pl.BlockSpec(memory_space=pl.ANY)] * 7,
        scratch_shapes=[
            dma((6, 2, long + 1)),
            dma((6, 2, long + 1)),
            dma((6, 2 * (long + 1))),
            dma((6, 2 * (long + 1))),
            dma((n,)),
            dma((n,)),
            dma((7,)),
        ],
        compiler_params=pltpu.CompilerParams(collective_id=0, has_side_effects=True),
    )(*shards, outgoing)


def outer_sum(columns, rows):
    total = columns[:, 0:1] * rows[0:1, :]
    for index in range(1, rows.shape[0]):
        total = total + columns[:, index : index + 1] * rows[index : index + 1, :]
    return total


def normalised(values):
    mean = jnp.mean(values, axis=0, keepdims=True)
    centred = values - mean
    var = jnp.mean(centred * centred, axis=0, keepdims=True)
    return centred * lax.rsqrt(var + norm_eps)


def nn(a, b):
    return jnp.dot(a, b, preferred_element_type=f32)


def nt(a, b):
    return lax.dot_general(a, b, (((1,), (1,)), ((), ())), preferred_element_type=f32)


def graph_kernel(
    block,
    count_ref,
    slot_ref,
    recv_ref,
    geom_ref,
    mesh_ref,
    arrived_ref,
    embed_ref,
    geom_cols_ref,
    mesh_cols_ref,
    film_ref,
    sender_ref,
    edge_ref,
    receiver_ref,
    message_ref,
    node_ref,
    output_ref,
    out_ref,
    table_ref,
    edge_t_ref,
    message_t_ref,
    embed_t_ref,
    total_ref,
):
    width = edge_ref.shape[1]
    listed = arrived_ref.shape[0]
    nodes = mesh_ref.shape[1]
    count = count_ref[0]
    edge_t_ref[...] = edge_ref[...].T
    message_t_ref[...] = message_ref[...].T
    received = silu(nt(embed_ref[...].T, arrived_ref[...])).astype(bf16)
    table_ref[:, :listed] = nn(sender_ref[...].T, received).astype(bf16)
    mesh_embed = silu(outer_sum(mesh_cols_ref[...], mesh_ref[...])).astype(bf16)
    embed_t_ref[...] = mesh_embed
    table_ref[:, listed:] = nn(receiver_ref[...].T, mesh_embed).astype(bf16)
    total_ref[...] = jnp.zeros_like(total_ref)

    @pl.loop(0, (count + block - 1) // block)
    def _(index):
        start = pl.multiple_of(index * block, block)
        here = pl.ds(start, block)
        slots = slot_ref[:, here]
        recv = recv_ref[:, here]
        live = start + lax.broadcasted_iota(jnp.int32, (1, block), 1) < count
        recv = jnp.where(live, recv, -1)
        pick = (lax.broadcasted_iota(jnp.int32, (listed, block), 0) == slots).astype(f32).astype(bf16)
        place = (lax.broadcasted_iota(jnp.int32, (nodes, block), 0) == recv).astype(f32).astype(bf16)
        embedded = silu(outer_sum(geom_cols_ref[...], geom_ref[:, here])).astype(bf16)
        pre = nn(edge_t_ref[...], embedded)
        pre = pre + nn(table_ref[:, :listed], pick)
        pre = pre + nn(table_ref[:, listed:], place)
        hidden = silu(pre).astype(bf16)
        mixed = nn(message_t_ref[...], hidden)
        message = normalised(mixed) * (1.0 + film_ref[:, 0:1]) + film_ref[:, 1:2]
        total_ref[...] += nt(message.astype(bf16), place)

    node_t = node_ref[...].T
    update = nn(node_t[:, :width], embed_t_ref[...])
    update = update + nn(node_t[:, width:], total_ref[...].astype(bf16))
    update = silu(update).astype(bf16)
    result = nn(output_ref[...].T, update)
    result = normalised(result) * (1.0 + film_ref[:, 2:3]) + film_ref[:, 3:4]
    out_ref[...] = (embed_t_ref[...].astype(f32) + result).T.astype(bf16)


def graph(count, slots, recv, geometry, features, arrived, embed, geom_cols, mesh_cols, film, weights):
    width = embed.shape[1]
    nodes = features.shape[1]
    edges = geometry.shape[1]
    listed = arrived.shape[0]
    block = min(512, edges)
    vmem = pl.BlockSpec(memory_space=pltpu.VMEM)
    return pl.pallas_call(
        functools.partial(graph_kernel, block),
        out_shape=jax.ShapeDtypeStruct((nodes, width), bf16),
        in_specs=[pl.BlockSpec(memory_space=pltpu.SMEM)] + [vmem] * 15,
        out_specs=vmem,
        scratch_shapes=[
            pltpu.VMEM((width, listed + nodes), bf16),
            pltpu.VMEM((width, width), bf16),
            pltpu.VMEM((width, width), bf16),
            pltpu.VMEM((width, nodes), bf16),
            pltpu.VMEM((width, nodes), f32),
        ],
    )(count, slots, recv, geometry, features, arrived, embed, geom_cols, mesh_cols, film, *weights)


def per_device(
    n,
    folded,
    conditioning,
    target_state,
    noise_sample,
    step_index,
    mesh_features,
    edge_geometry,
    edge_slot,
    edge_receiver,
    send_rows,
    edge_count,
    embed_weight,
    mesh_weight,
    geom_weight,
    sender_weight,
    edge_weight,
    receiver_weight,
    message_weight,
    node_weight,
    output_weight,
    noise_weight,
    film_weight,
):
    width = embed_weight.shape[1]
    freqs = noise_weight.shape[0] // 2
    steps_total = STEPS
    frac = step_index[0].astype(jnp.float32) / (steps_total - 1)
    upper = sigma_top ** (1.0 / rho_power)
    lower = sigma_low ** (1.0 / rho_power)
    sigma = (upper + frac * (lower - upper)) ** rho_power
    angle = 0.25 * jnp.log(sigma) * (jnp.arange(freqs, dtype=jnp.float32) + 1.0)
    fourier = jnp.concatenate([jnp.sin(angle), jnp.cos(angle)])[None, :]
    cond = jax.nn.silu(jnp.dot(fourier, noise_weight, precision=lax.Precision.HIGHEST)).astype(
        jnp.bfloat16
    )
    film = jnp.dot(cond, film_weight, preferred_element_type=f32)
    film = film.reshape(4, width).T
    noisy = ((target_state + sigma * noise_sample) / jnp.sqrt(sigma * sigma + 1.0)).astype(bf16)
    channels = embed_weight.shape[0]
    spare = -channels % 128
    points = conditioning.shape[1]
    raw_local = jnp.concatenate([conditioning, noisy], axis=0)
    raw_local = jnp.pad(raw_local, ((0, spare), (0, 0)))
    embed = jnp.pad(embed_weight, ((0, spare), (0, 0)))
    picked = (send_rows.reshape(-1)[:, None] == jnp.arange(points, dtype=jnp.int32)[None, :]).astype(bf16)
    outgoing = nt(picked, raw_local).astype(bf16)
    cap = send_rows.shape[1]
    outgoing = outgoing.reshape(n, cap, channels + spare)
    shards = (sender_weight, edge_weight, receiver_weight, message_weight, node_weight, output_weight)
    *fulls, arrived = exchange(n, folded, shards, outgoing)
    weights = [full.reshape(-1, width) for full in fulls]
    return graph(
        edge_count,
        edge_slot.reshape(1, -1),
        edge_receiver.reshape(1, -1),
        edge_geometry,
        mesh_features,
        arrived.reshape(n * cap, channels + spare),
        embed,
        geom_weight.T,
        mesh_weight.T,
        film,
        weights,
    )


def solution(mesh):
    placed = (
        P(None, ("member", "node")),
        P(None, ("member", "node")),
        P(None, ("member", "node")),
        P("member"),
        P(None, "node"),
        P(None, "node"),
        P("node"),
        P("node"),
        P("node", None),
        P("node"),
        P(),
        P(),
        P(),
        P("node", None),
        P("node", None),
        P("node", None),
        P("node", None),
        P("node", None),
        P("node", None),
        P(),
        P(),
    )
    n = mesh.shape["node"]
    body = functools.partial(per_device, n, is_folded(mesh))
    return jax.shard_map(
        body, mesh=mesh, in_specs=placed, out_specs=P("node", "member"), check_vma=False
    )
```

```python
import functools

import jax
import jax.numpy as jnp
from jax import lax
from jax.experimental import pallas as pl
from jax.experimental.pallas import tpu as pltpu
from jax.sharding import PartitionSpec as P

STEPS = 20


sigma_top = 80.0
sigma_low = 0.03
rho_power = 7.0
norm_eps = 1e-05
f32, bf16 = jnp.float32, jnp.bfloat16


def is_folded(mesh):
    rows = mesh.devices[0]
    places = [getattr(device, "coords", None) for device in rows[:5:2]]
    if len(places) < 3 or any(place is None for place in places):
        return False
    first = [a != b for a, b in zip(places[0], places[1])]
    second = [a != b for a, b in zip(places[0], places[2])]
    return first != second


def silu(x):
    half = 0.5 * x
    return half * jnp.tanh(half) + half


def outer_sum(columns, rows):
    total = columns[:, 0:1] * rows[0:1, :]
    for index in range(1, rows.shape[0]):
        total = total + columns[:, index : index + 1] * rows[index : index + 1, :]
    return total


def normalised(values):
    mean = jnp.mean(values, axis=0, keepdims=True)
    centred = values - mean
    var = jnp.mean(centred * centred, axis=0, keepdims=True)
    return centred * lax.rsqrt(var + norm_eps)


def nn(a, b):
    return jnp.dot(a, b, preferred_element_type=f32)


def nt(a, b):
    return lax.dot_general(a, b, (((1,), (1,)), ((), ())), preferred_element_type=f32)


def encoder_kernel(n, folded, block, *refs):
    step_ref, count_ref, slot_ref, recv_ref, rows_ref, geom_ref, mesh_ref = refs[:7]
    cond_ref, target_ref, noise_ref, embed_ref, mesh_w_ref, geom_w_ref, noise_w_ref, film_w_ref = refs[7:15]
    shards, out_ref = refs[15:21], refs[21]
    fulls = refs[22:28]
    picked_ref, outgoing, arrived, embed_pad_ref, cols_ref, edges_ref = refs[28:34]
    table_ref, edge_t_ref, message_t_ref, embed_t_ref, total_ref = refs[34:39]
    send_sem, recv_sem, psend_sem, precv_sem, asend_sem, arecv_sem, own_sem = refs[39:]
    me = lax.axis_index("node")
    core, chip = me % 2, me // 2
    partner = chip * 2 + 1 - core
    chips = n // 2
    half = chips // 2

    def same(index):
        return index

    if folded:

        def to_pos(c):
            z, y = c // 2, c % 2
            return z + y * (chips - 1 - 2 * z)

        def to_chip(p):
            y = p // half
            return (p + y * (chips - 1 - 2 * p)) * 2 + y
    else:
        to_pos = to_chip = same

    pos = to_pos(chip)

    def device_at(shift):
        return to_chip((pos + shift + chips) % chips) * 2 + core

    sent = []

    def remote(source, target, send, recv, device):
        copy = pltpu.make_async_remote_copy(
            src_ref=source, dst_ref=target, send_sem=send, recv_sem=recv, device_id={"node": device}
        )
        copy.start()
        sent.append(copy)
        return copy

    long, short = chips // 2, chips - 1 - chips // 2
    reach = [[long, short] if k % 2 == 0 else [short, long] for k in range(6)]
    ring = {}
    passed = {k: [] for k in range(6)}
    early, late = (0, 1, 2, 3), (4, 5)

    def relay(group, step):
        onward = []
        for k in group:
            for side in (0, 1):
                way = 1 - 2 * side
                last = reach[k][side]
                if step > last + 1:
                    continue
                block_at = device_at(-way * (step - 1))
                target = fulls[k].at[block_at]
                source = shards[k] if step == 1 else target
                if step > 1:
                    ring[k, side, step - 1].wait_recv()
                if step <= last:
                    ring[k, side, step] = remote(
                        source,
                        target,
                        send_sem.at[k, side, step],
                        recv_sem.at[k, side, step],
                        device_at(way),
                    )
                if step > 1 or side == 0:
                    index = side * (long + 1) + step - 1
                    onward.append((k, index, source, target))
        for k, index, source, target in onward:
            passed[k].append(
                remote(source, target, psend_sem.at[k, index], precv_sem.at[k, index], partner)
            )

    barrier = pltpu.get_barrier_semaphore()
    for step in range(1, n):
        pl.semaphore_signal(barrier, inc=1, device_id={"node": (me + step) % n})
    own = []
    for k in range(6):
        own.append(pltpu.make_async_copy(shards[k], fulls[k].at[me], own_sem.at[k]))
        own[k].start()
    pl.semaphore_wait(barrier, n - 1)
    relay(early, 1)

    width = embed_ref.shape[1]
    channels = embed_ref.shape[0]
    cap = outgoing.shape[1]
    frac = jnp.full((1, 1), step_ref[0], jnp.int32).astype(f32) / (STEPS - 1)
    upper = sigma_top ** (1.0 / rho_power)
    lower = sigma_low ** (1.0 / rho_power)
    root = upper + frac * (lower - upper)
    cube = root * root * root
    sigma = cube * cube * root
    noisy = ((target_ref[...] + sigma * noise_ref[...]) / jnp.sqrt(sigma * sigma + 1.0)).astype(bf16)
    points, listed = cond_ref.shape[1], rows_ref.shape[1]
    fixed = cond_ref.shape[0]
    pick = lax.broadcasted_iota(jnp.int32, (points, listed), 0) == rows_ref[...]
    pick = pick.astype(f32).astype(bf16)
    picked_ref[...] = jnp.zeros_like(picked_ref)
    picked_ref[:fixed, :] = nn(cond_ref[...], pick)
    picked_ref[fixed:channels, :] = nn(noisy, pick)
    outgoing[...] = picked_ref[...].T.astype(bf16).reshape(outgoing.shape)
    relay(early, 2)

    freqs = noise_w_ref.shape[0] // 2
    place_k = lax.broadcasted_iota(jnp.int32, (2 * freqs, 1), 0)
    wave = (place_k % freqs + 1).astype(f32)
    angle = 0.25 * jnp.log(sigma) * wave
    fourier = jnp.where(place_k < freqs, jnp.sin(angle), jnp.cos(angle))
    cond = silu(jnp.sum(fourier * noise_w_ref[...], axis=0, keepdims=True)).astype(bf16)
    film = nn(cond, film_w_ref[...])
    small = [film[:, width * i : width * (i + 1)] for i in range(4)]
    geoms, feats = geom_w_ref.shape[0], mesh_w_ref.shape[0]
    small += [geom_w_ref[i : i + 1, :] for i in range(geoms)]
    small += [mesh_w_ref[i : i + 1, :] for i in range(feats)]
    line = lax.broadcasted_iota(jnp.int32, (128, width), 0)
    stacked = jnp.zeros((128, width), f32)
    for i, row in enumerate(small):
        stacked = jnp.where(line == i, row, stacked)
    cols_ref[...] = stacked.T
    geom_cols = cols_ref[:, 4 : 4 + geoms]
    mesh_cols = cols_ref[:, 4 + geoms : 4 + geoms + feats]
    mesh_embed = silu(outer_sum(mesh_cols, mesh_ref[...])).astype(bf16)
    embed_t_ref[...] = mesh_embed

    own.append(pltpu.make_async_copy(outgoing.at[me], arrived.at[me], own_sem.at[6]))
    own[6].start()
    swaps = []
    for step in range(1, n):
        other = (me + step) % n
        swaps.append(
            remote(outgoing.at[other], arrived.at[me], asend_sem.at[step], arecv_sem.at[step], other)
        )
    relay(early, 3)
    relay(late, 1)

    blocks = geom_ref.shape[1] // block

    def embed_edges(index, carry):
        here = pl.ds(pl.multiple_of(index * block, block), block)
        edges_ref[index] = silu(outer_sum(geom_cols, geom_ref[:, here])).astype(bf16)
        return carry

    lax.fori_loop(0, blocks // 2, embed_edges, 0)
    relay(early, 4)
    lax.fori_loop(blocks // 2, blocks, embed_edges, 0)
    for step in range(5, long + 2):
        relay(early, step)
    embed_pad_ref[...] = jnp.zeros_like(embed_pad_ref)
    embed_pad_ref[:channels, :] = embed_ref[...]
    for copy in own:
        copy.wait()
    for copy in swaps:
        copy.wait_recv()
    sources = arrived[...].reshape(listed, arrived.shape[2])
    received = silu(nt(embed_pad_ref[...].T, sources)).astype(bf16)

    def full(k):
        return fulls[k][...].reshape(-1, width)

    for k in early:
        for copy in passed[k]:
            copy.wait_recv()
    table_ref[:, :listed] = nn(full(0).T, received).astype(bf16)
    edge_t_ref[...] = full(1).T
    table_ref[:, listed:] = nn(full(2).T, embed_t_ref[...]).astype(bf16)
    message_t_ref[...] = full(3).T
    total_ref[...] = jnp.zeros_like(total_ref)
    nodes = mesh_ref.shape[1]
    count = count_ref[0]

    def add_block(index, carry):
        start = pl.multiple_of(index * block, block)
        here = pl.ds(start, block)
        recv = recv_ref[:, here]
        live = start + lax.broadcasted_iota(jnp.int32, (1, block), 1) < count
        recv = jnp.where(live, recv, -1)
        pick = lax.broadcasted_iota(jnp.int32, (listed, block), 0) == slot_ref[:, here]
        pick = pick.astype(f32).astype(bf16)
        place = lax.broadcasted_iota(jnp.int32, (nodes, block), 0) == recv
        place = place.astype(f32).astype(bf16)
        pre = nn(edge_t_ref[...], edges_ref[index])
        pre = pre + nn(table_ref[:, :listed], pick)
        pre = pre + nn(table_ref[:, listed:], place)
        hidden = silu(pre).astype(bf16)
        mixed = nn(message_t_ref[...], hidden)
        message = normalised(mixed) * (1.0 + cols_ref[:, 0:1]) + cols_ref[:, 1:2]
        total_ref[...] += nt(message.astype(bf16), place)
        return carry

    stages = min(long, blocks)
    for stage in range(stages):
        lax.fori_loop(blocks * stage // stages, blocks * (stage + 1) // stages, add_block, 0)
        relay(late, stage + 2)
    for step in range(stages + 2, long + 2):
        relay(late, step)
    for k in late:
        for copy in passed[k]:
            copy.wait_recv()
    node_t = full(4).T
    update = nn(node_t[:, :width], embed_t_ref[...])
    update = update + nn(node_t[:, width:], total_ref[...].astype(bf16))
    update = silu(update).astype(bf16)
    result = nn(full(5).T, update)
    result = normalised(result) * (1.0 + cols_ref[:, 2:3]) + cols_ref[:, 3:4]
    out_ref[...] = (embed_t_ref[...].astype(f32) + result).T.astype(bf16)
    for copy in sent:
        copy.wait_send()


def per_device(n, folded, *args):
    conditioning, target_state, noise_sample, step_index, mesh_features, edge_geometry = args[:6]
    edge_slot, edge_receiver, send_rows, edge_count, embed_weight, mesh_weight, geom_weight = args[6:13]
    shards, noise_weight, film_weight = args[13:19], args[19], args[20]
    channels, width = embed_weight.shape
    nodes, edges = mesh_features.shape[1], edge_geometry.shape[1]
    cap = send_rows.shape[1]
    listed = n * cap
    deep = channels + -channels % 128
    block = min(512, edges)
    long = n // 4 + 1
    dma = pltpu.SemaphoreType.DMA
    vmem = pl.BlockSpec(memory_space=pltpu.VMEM)
    smem = pl.BlockSpec(memory_space=pltpu.SMEM)
    return pl.pallas_call(
        functools.partial(encoder_kernel, n, folded, block),
        out_shape=jax.ShapeDtypeStruct((nodes, width), bf16),
        in_specs=[smem] * 2 + [vmem] * 19,
        out_specs=vmem,
        scratch_shapes=[pltpu.VMEM((n,) + shard.shape, bf16) for shard in shards]
        + [
            pltpu.VMEM((deep, listed), f32),
            pltpu.VMEM((n, cap, deep), bf16),
            pltpu.VMEM((n, cap, deep), bf16),
            pltpu.VMEM((deep, width), bf16),
            pltpu.VMEM((width, 128), f32),
            pltpu.VMEM((edges // block, width, block), bf16),
            pltpu.VMEM((width, listed + nodes), bf16),
            pltpu.VMEM((width, width), bf16),
            pltpu.VMEM((width, width), bf16),
            pltpu.VMEM((width, nodes), bf16),
            pltpu.VMEM((width, nodes), f32),
            dma((6, 2, long + 1)),
            dma((6, 2, long + 1)),
            dma((6, 2 * (long + 1))),
            dma((6, 2 * (long + 1))),
            dma((n,)),
            dma((n,)),
            dma((7,)),
        ],
        compiler_params=pltpu.CompilerParams(collective_id=0, has_side_effects=True),
    )(
        step_index,
        edge_count,
        edge_slot.reshape(1, -1),
        edge_receiver.reshape(1, -1),
        send_rows.reshape(1, -1),
        edge_geometry,
        mesh_features,
        conditioning,
        target_state,
        noise_sample,
        embed_weight,
        mesh_weight,
        geom_weight,
        noise_weight,
        film_weight,
        *shards,
    )


def solution(mesh):
    placed = (
        P(None, ("member", "node")),
        P(None, ("member", "node")),
        P(None, ("member", "node")),
        P("member"),
        P(None, "node"),
        P(None, "node"),
        P("node"),
        P("node"),
        P("node", None),
        P("node"),
        P(),
        P(),
        P(),
        P("node", None),
        P("node", None),
        P("node", None),
        P("node", None),
        P("node", None),
        P("node", None),
        P(),
        P(),
    )
    n = mesh.shape["node"]
    body = functools.partial(per_device, n, is_folded(mesh))
    return jax.shard_map(
        body, mesh=mesh, in_specs=placed, out_specs=P("node", "member"), check_vma=False
    )
```
